32 devices in a mesh: grp: 2 (over x), seq: 8 (over z, y), kv: 2 (over core).
Axes of the slice: x: 2, y: 2, z: 4, core: 2. Of those that a mesh axis runs over, the one named last changes fastest.
Arguments:
- queries: bfloat16 [4, 64, 128], P(('grp', 'kv'), 'seq'), parts along dimension 0, may hold values from -256 to 256
- keys: bfloat16 [4, 16384, 8, 128], P(('grp', 'kv'), 'seq'), parts along dimension 0, may hold values from -6 to 6
- values: bfloat16 [4, 16384, 8, 128], P(('grp', 'kv'), 'seq'), parts along dimension 0, may hold values from -6 to 6
- picks: int32 [4, 64, 3], P(('grp', 'kv'), 'seq'), parts along dimension 0, may hold values from 0 to 31, as said below
- lengths: int32 [4], P(('grp', 'kv')), parts along dimension 0, may hold values from 8194 to 16384, as said below
Outputs:
- attended: bfloat16 [4, 64, 128], P(('grp', 'kv'), 'seq'), parts along dimension 0
The draws below stay inside these ranges and needn't reach their ends.
There are 2 independent parts, one for each index of `grp`. The reference program is written for one: setup_inputs(seed, part) draws one part's arguments, and reference() takes and returns one part's arrays. A program takes and returns all parts, laid end to end along the dimension named above; each array names one. Nothing has to cross between parts.
Inputs may be any that keep to these rules, and one draw needn't show every extreme that they name: `picks`: each row of 3 holds distinct block numbers in ascending order; the last is the block that holds position lengths[b] - 1, the others lie before it. Position lengths[b] - 1 is never the first position of its block.
All inputs are finite; a program needn't handle non-finite values.
Results may differ from the reference program's by a relative error of at most 0.0046.
Values may be sent and summed in bfloat16 or wider, within the bound.
A program may use at most 64 MiB of HBM per device.

```python
import math
import jax
import jax.numpy as jnp
from jax import lax

HD = 128
QH = 64
KVH = 8
BATCH = 2
BLOCK = 512
NBLK = 32
CTX = 16384


def block_keys(key, row, block):
    inner = jax.random.fold_in(jax.random.fold_in(jax.random.fold_in(key, 101), row), block)
    return jnp.clip(jax.random.normal(inner, (BLOCK, KVH, HD), jnp.float32), -6.0, 6.0)


def context_parts(key):
    inner = jax.random.fold_in(key, 202)
    current = jax.random.randint(jax.random.fold_in(inner, 1), (BATCH,), NBLK // 2, NBLK)
    offset = jax.random.randint(jax.random.fold_in(inner, 2), (BATCH,), 2, BLOCK + 1)
    row_ids = jnp.arange(BATCH, dtype=jnp.int32)
    current = jnp.where(row_ids == 0, NBLK - 1, current)
    current = jnp.where(row_ids == 1, NBLK // 2, current)
    return (current.astype(jnp.int32), offset.astype(jnp.int32))


def draw_keys(key, part):
    blocks = jnp.arange(NBLK, dtype=jnp.int32)

    def whole_row(row):
        return jax.vmap(lambda block: block_keys(key, row, block))(blocks)
    whole = jax.vmap(whole_row)(jnp.arange(BATCH, dtype=jnp.int32))
    return whole.reshape(BATCH, NBLK * BLOCK, KVH, HD).astype(jnp.bfloat16)


def draw_lengths(key, part):
    current, offset = context_parts(key)
    return (current * BLOCK + offset).astype(jnp.int32)


def draw_picks(key, part):
    current, offset = context_parts(key)
    inner = jax.random.fold_in(key, 303)
    upper = current[:, None]
    factor_one = jax.random.randint(jax.random.fold_in(inner, 1), (BATCH, QH), 0, upper)
    factor_two = jax.random.randint(jax.random.fold_in(inner, 2), (BATCH, QH), 0, upper)
    first = factor_one * factor_two // upper
    second = jax.random.randint(jax.random.fold_in(inner, 3), (BATCH, QH), 0, upper - 1)
    second = second + (second >= first).astype(jnp.int32)
    lower = jnp.minimum(first, second)
    higher = jnp.maximum(first, second)
    latest = jnp.broadcast_to(upper, (BATCH, QH))
    return jnp.stack([lower, higher, latest], axis=-1).astype(jnp.int32)


def draw_queries(key, part):
    base = jax.random.fold_in(key, 404)
    result = jnp.clip(jax.random.normal(jax.random.fold_in(base, 5), (BATCH, QH, HD), jnp.float32), -6.0, 6.0)
    return jnp.clip(result, -256.0, 256.0).astype(jnp.bfloat16)


def level_of(rng, extent, split, least, largest):
    level, own = 1.0, jax.random.fold_in(rng, 6)
    for position, blocks in split:
        draws = jnp.exp(jax.random.uniform(jax.random.fold_in(own, position), (blocks,), jnp.float32, least / len(split), largest / len(split)))
        level = level * jnp.repeat(draws, extent[position] // blocks).reshape([-1 if axis == position else 1 for axis in range(len(extent))])
    return level


def normal_values(own_key, dims, spread, reach, pieces=(), held_as=jnp.bfloat16):
    entries = spread * jax.random.normal(own_key, dims, jnp.float32)
    if pieces:
        entries = entries * level_of(own_key, dims, pieces, -0.22, 0.18)
    return jnp.clip(entries, -reach, reach).astype(held_as)


def setup_inputs(seed: int = 0, part: int = 0) -> dict:
    arg_keys = jax.random.split(jax.random.key(seed), 6)
    own_keys = jax.random.split(jax.random.fold_in(arg_keys[5], part), 6)
    queries = draw_queries(jax.random.fold_in(jax.random.fold_in(arg_keys[5], part), 71), part)
    keys = draw_keys(jax.random.fold_in(jax.random.fold_in(arg_keys[5], part), 71), part)
    values = normal_values(own_keys[2], (BATCH, CTX, KVH, HD), 1.0, 6.0, ((0, 2), (1, 8)))
    picks = draw_picks(jax.random.fold_in(jax.random.fold_in(arg_keys[5], part), 71), part)
    lengths = draw_lengths(jax.random.fold_in(jax.random.fold_in(arg_keys[5], part), 71), part)
    return {"queries": queries, "keys": keys, "values": values, "picks": picks, "lengths": lengths}


def one_row(query_row, key_row, value_row, pick_row, length):
    key_blocks = key_row.reshape(NBLK, BLOCK, KVH, HD)
    value_blocks = value_row.reshape(NBLK, BLOCK, KVH, HD)
    offsets = jnp.arange(BLOCK, dtype=jnp.int32)
    group = QH // KVH

    def one_head(item):
        query, chosen, head = item
        kv_head = (head // group).astype(jnp.int32)
        keys_here = lax.dynamic_index_in_dim(jnp.take(key_blocks, chosen, axis=0), kv_head, axis=2, keepdims=False)
        values_here = lax.dynamic_index_in_dim(jnp.take(value_blocks, chosen, axis=0), kv_head, axis=2, keepdims=False)
        scores = jnp.einsum('d,jtd->jt', query.astype(jnp.float32), keys_here.astype(jnp.float32)) * (1.0 / math.sqrt(HD))
        positions = chosen[:, None] * BLOCK + offsets[None, :]
        live = positions < length
        masked = jnp.where(live, scores, -jnp.inf)
        block_max = lax.optimization_barrier(jnp.max(masked, axis=-1))
        weight = jnp.exp(masked - block_max[:, None])
        block_total = lax.optimization_barrier(jnp.sum(weight, axis=-1))
        rounded = weight.astype(jnp.bfloat16)
        block_out = jnp.einsum('jt,jtd->jd', rounded.astype(jnp.float32), values_here.astype(jnp.float32))
        top = jnp.max(block_max)
        coef = jnp.exp(block_max - top)
        return lax.optimization_barrier(jnp.sum(coef[:, None] * block_out, axis=0)) / jnp.sum(coef * block_total)
    heads = jnp.arange(QH, dtype=jnp.int32)
    return lax.map(one_head, (query_row, pick_row, heads)).astype(jnp.bfloat16)

def reference(queries, keys, values, picks, lengths):
    outputs = []
    for row in range(BATCH):
        outputs.append(one_row(queries[row], keys[row], values[row], picks[row], lengths[row]))
    return jnp.stack(outputs, axis=0)
```

```python
import functools
import math

import jax
import jax.numpy as jnp
from jax import lax
from jax.experimental import pallas as pl
from jax.experimental.pallas import tpu as pltpu
from jax.sharding import PartitionSpec as P

BLOCK = 512
CHUNK = 512
NEGATIVE = -1e30


def kernel(
    n,
    kv_heads,
    lengths_ref,
    q_ref,
    picks_ref,
    k_hbm,
    v_hbm,
    out_ref,
    kbuf,
    vbuf,
    qbuf,
    pbuf,
    qall,
    pall,
    bias,
    sbuf,
    msg,
    came,
    k_sem,
    v_sem,
    own_sem,
    q_send,
    q_recv,
    p_send,
    p_recv,
    m_send,
    m_recv,
):
    me = lax.axis_index("seq")
    hl, hd = q_ref.shape[1], q_ref.shape[2]
    heads = n * hl
    group = heads // kv_heads
    span = BLOCK * kv_heads
    blocks_here = k_hbm.shape[0] // span
    factor = math.log2(math.e) / math.sqrt(hd)

    barrier = pltpu.get_barrier_semaphore()
    for d in range(1, n):
        pl.semaphore_signal(
            barrier, inc=1, device_id={"seq": lax.rem(me + d, n)}, device_id_type=pl.DeviceIdType.MESH
        )
    k_copies, v_copies = [], []
    for b in range(blocks_here):
        rows = pl.ds(b * span, span)
        k_copies.append(pltpu.make_async_copy(k_hbm.at[rows], kbuf.at[rows], k_sem.at[b]))
        v_copies.append(pltpu.make_async_copy(v_hbm.at[rows], vbuf.at[rows], v_sem.at[b]))
    for c in k_copies:
        c.start()
    own_q = pltpu.make_async_copy(q_ref.at[0], qbuf.at[me], own_sem.at[0])
    own_p = pltpu.make_async_copy(picks_ref.at[0], pbuf.at[me], own_sem.at[1])
    own_q.start()
    own_p.start()
    for c in v_copies:
        c.start()
    pl.semaphore_wait(barrier, n - 1)

    sends = []
    for d in range(1, n):
        peer = {"seq": lax.rem(me + d, n)}
        for src, dst, s_sem, r_sem in (
            (q_ref.at[0], qbuf.at[me], q_send.at[d], q_recv.at[d]),
            (picks_ref.at[0], pbuf.at[me], p_send.at[d], p_recv.at[d]),
        ):
            c = pltpu.make_async_remote_copy(
                src_ref=src,
                dst_ref=dst,
                send_sem=s_sem,
                recv_sem=r_sem,
                device_id=peer,
                device_id_type=pl.DeviceIdType.MESH,
            )
            c.start()
            sends.append(c)
    own_q.wait()
    own_p.wait()
    for c in sends:
        c.wait_recv()

    for p in range(n):
        qall[p * hl : (p + 1) * hl, :] = qbuf[p].astype(jnp.float32)
        pall[p * hl : (p + 1) * hl, :] = pbuf[p]
    q = qall[...].astype(jnp.bfloat16)
    picks = pall[...]
    length = lengths_ref[0]

    lane = lax.broadcasted_iota(jnp.int32, (heads, 128), 1)
    row = lax.broadcasted_iota(jnp.int32, (heads, 128), 0)
    mine = (lane % kv_heads) == (row // group)
    for b in range(blocks_here):
        block_id = me * blocks_here + b
        chosen = jnp.max((picks == block_id).astype(jnp.int32), axis=1, keepdims=True)
        ok = jnp.logical_and(mine, jnp.broadcast_to(chosen, (heads, 128)) > 0)
        bias[b] = jnp.where(ok, 0.0, NEGATIVE)

    reps = CHUNK // 128
    col = lax.broadcasted_iota(jnp.int32, (1, CHUNK), 1) // kv_heads
    dims = (((1,), (1,)), ((), ()))
    top = jnp.full((heads, 128), 3 * NEGATIVE, jnp.float32)
    for b in range(blocks_here):
        k_copies[b].wait()
        start = (me * blocks_here + b) * BLOCK
        for j in range(span // CHUNK):
            lo = b * span + j * CHUNK
            s = lax.dot_general(q, kbuf[lo : lo + CHUNK, :], dims, preferred_element_type=jnp.float32)
            end = jnp.where(col + (start + j * (CHUNK // kv_heads)) < length, 0.0, NEGATIVE)
            for r in range(reps):
                part = s[:, r * 128 : (r + 1) * 128] + (bias[b] + end[:, r * 128 : (r + 1) * 128])
                top = jnp.maximum(top, part)
                sbuf[:, lo + r * 128 : lo + (r + 1) * 128] = part
    high = jnp.max(top, axis=1, keepdims=True)
    high_wide = jnp.broadcast_to(high, (heads, 128))

    total = jnp.zeros((heads, 128), jnp.float32)
    acc = jnp.zeros((heads, hd), jnp.float32)
    for b in range(blocks_here):
        v_copies[b].wait()
        for j in range(span // CHUNK):
            lo = b * span + j * CHUNK
            pieces = []
            for r in range(reps):
                w = jnp.exp2((sbuf[:, lo + r * 128 : lo + (r + 1) * 128] - high_wide) * factor)
                total = total + w
                pieces.append(w.astype(jnp.bfloat16))
            acc = acc + jnp.dot(
                jnp.concatenate(pieces, axis=1), vbuf[lo : lo + CHUNK, :], preferred_element_type=jnp.float32
            )
    total_wide = jnp.broadcast_to(jnp.sum(total, axis=1, keepdims=True), (heads, 128))
    half = lax.broadcasted_iota(jnp.int32, (heads, 128), 1) < 64
    stats = jnp.where(half, high_wide, total_wide)
    for p in range(n):
        msg[p, 0] = acc[p * hl : (p + 1) * hl, :]
        msg[p, 1] = stats[p * hl : (p + 1) * hl, :]
    backs = []
    for d in range(1, n):
        peer = lax.rem(me + d, n)
        c = pltpu.make_async_remote_copy(
            src_ref=msg.at[peer],
            dst_ref=came.at[me],
            send_sem=m_send.at[d],
            recv_sem=m_recv.at[d],
            device_id={"seq": peer},
            device_id_type=pl.DeviceIdType.MESH,
        )
        c.start()
        backs.append(c)
    came[me] = msg[me]
    for c in sends:
        c.wait_send()
    for c in backs:
        c.wait_recv()
    best = came[0, 1]
    for p in range(1, n):
        best = jnp.maximum(best, came[p, 1])
    best = jnp.broadcast_to(best[:, 0:1], (hl, 128))
    sum_out = jnp.zeros((hl, hd), jnp.float32)
    sum_total = jnp.zeros((hl, 128), jnp.float32)
    for p in range(n):
        st = came[p, 1]
        scale = jnp.exp2((jnp.broadcast_to(st[:, 0:1], (hl, 128)) - best) * factor)
        sum_out = sum_out + came[p, 0] * scale
        sum_total = sum_total + jnp.broadcast_to(st[:, 64:65], (hl, 128)) * scale
    out_ref[0] = (sum_out / sum_total).astype(out_ref.dtype)
    for c in backs:
        c.wait_send()


def shards(n, queries, keys, values, picks, lengths):
    _, hl, hd = queries.shape
    _, local_len, kv_heads, _ = keys.shape
    heads = n * hl
    cols = local_len * kv_heads
    blocks_here = local_len // BLOCK
    k2 = keys.reshape(cols, hd)
    v2 = values.reshape(cols, hd)
    any_space = pl.BlockSpec(memory_space=pl.ANY)
    sems = [pltpu.SemaphoreType.DMA((n,)) for _ in range(6)]
    return pl.pallas_call(
        functools.partial(kernel, n, kv_heads),
        out_shape=jax.ShapeDtypeStruct((1, hl, hd), jnp.bfloat16),
        in_specs=[pl.BlockSpec(memory_space=pltpu.SMEM)] + [any_space] * 4,
        out_specs=pl.BlockSpec(memory_space=pltpu.VMEM),
        scratch_shapes=[
            pltpu.VMEM((cols, hd), jnp.bfloat16),
            pltpu.VMEM((cols, hd), jnp.bfloat16),
            pltpu.VMEM((n, hl, hd), jnp.bfloat16),
            pltpu.VMEM((n, hl, picks.shape[2]), jnp.int32),
            pltpu.VMEM((heads, hd), jnp.float32),
            pltpu.VMEM((heads, picks.shape[2]), jnp.int32),
            pltpu.VMEM((blocks_here, heads, 128), jnp.float32),
            pltpu.VMEM((heads, cols), jnp.float32),
            pltpu.VMEM((n, 2, hl, 128), jnp.float32),
            pltpu.VMEM((n, 2, hl, 128), jnp.float32),
            pltpu.SemaphoreType.DMA((blocks_here,)),
            pltpu.SemaphoreType.DMA((blocks_here,)),
            pltpu.SemaphoreType.DMA((2,)),
        ]
        + sems,
        compiler_params=pltpu.CompilerParams(collective_id=0, has_side_effects=True),
        name="block_attention",
    )(lengths, queries, picks, k2, v2)


def solution(mesh):
    return jax.shard_map(
        functools.partial(shards, mesh.shape["seq"]),
        mesh=mesh,
        in_specs=(
            P(("grp", "kv"), "seq", None),
            P(("grp", "kv"), "seq", None, None),
            P(("grp", "kv"), "seq", None, None),
            P(("grp", "kv"), "seq", None),
            P(("grp", "kv")),
        ),
        out_specs=P(("grp", "kv"), "seq", None),
        check_vma=False,
    )
```

```python
import functools
import math

import jax
import jax.numpy as jnp
from jax import lax
from jax.experimental import pallas as pl
from jax.experimental.pallas import tpu as pltpu
from jax.sharding import PartitionSpec as P

BLOCK = 512
CHUNK = 512
NEGATIVE = -1e30


def kernel(
    n,
    kv_heads,
    lengths_ref,
    q_ref,
    picks_ref,
    k_hbm,
    v_hbm,
    out_ref,
    kbuf,
    vbuf,
    qbuf,
    pbuf,
    qall,
    pall,
    lbuf,
    bias,
    sbuf,
    msg,
    came,
    k_sem,
    v_sem,
    own_sem,
    q_send,
    q_recv,
    p_send,
    p_recv,
    m_send,
    m_recv,
):
    me = lax.axis_index("seq")
    hl, hd = q_ref.shape[1], q_ref.shape[2]
    heads = n * hl
    group = heads // kv_heads
    span = BLOCK * kv_heads
    blocks_here = k_hbm.shape[0] // span
    factor = math.log2(math.e) / math.sqrt(hd)

    barrier = pltpu.get_barrier_semaphore()
    for d in range(1, n):
        pl.semaphore_signal(
            barrier, inc=1, device_id={"seq": lax.rem(me + d, n)}, device_id_type=pl.DeviceIdType.MESH
        )
    k_copies, v_copies = [], []
    for b in range(blocks_here):
        rows = pl.ds(b * span, span)
        k_copies.append(pltpu.make_async_copy(k_hbm.at[rows], kbuf.at[rows], k_sem.at[b]))
        v_copies.append(pltpu.make_async_copy(v_hbm.at[rows], vbuf.at[rows], v_sem.at[b]))
    for c in k_copies:
        c.start()
    own_q = pltpu.make_async_copy(q_ref.at[0], qbuf.at[me], own_sem.at[0])
    own_p = pltpu.make_async_copy(picks_ref, pbuf.at[me], own_sem.at[1])
    own_l = pltpu.make_async_copy(lengths_ref, lbuf, own_sem.at[2])
    own_q.start()
    own_p.start()
    own_l.start()
    for c in v_copies:
        c.start()
    pall[...] = jnp.full(pall.shape, -1, jnp.int32)
    own_q.wait()
    own_p.wait()
    own_l.wait()
    pl.semaphore_wait(barrier, n - 1)

    sends = []
    for d in range(1, n):
        peer = {"seq": lax.rem(me + d, n)}
        for src, dst, s_sem, r_sem in (
            (qbuf.at[me], qbuf.at[me], q_send.at[d], q_recv.at[d]),
            (pbuf.at[me], pbuf.at[me], p_send.at[d], p_recv.at[d]),
        ):
            c = pltpu.make_async_remote_copy(
                src_ref=src,
                dst_ref=dst,
                send_sem=s_sem,
                recv_sem=r_sem,
                device_id=peer,
                device_id_type=pl.DeviceIdType.MESH,
            )
            c.start()
            sends.append(c)
    for c in sends:
        c.wait_recv()

    for p in range(n):
        qall[p * hl : (p + 1) * hl, :] = qbuf[p].astype(jnp.float32)
        pall[0 : pbuf.shape[1], p * hl : (p + 1) * hl] = pbuf[p, :, 0, :]
    q = qall[...].astype(jnp.bfloat16)
    picks = jnp.transpose(pall[...])[0:heads, :]
    length = lbuf[0]

    lane = lax.broadcasted_iota(jnp.int32, (heads, 128), 1)
    row = lax.broadcasted_iota(jnp.int32, (heads, 128), 0)
    mine = (lane % kv_heads) == (row // group)
    for b in range(blocks_here):
        block_id = me * blocks_here + b
        chosen = jnp.max((picks == block_id).astype(jnp.int32), axis=1, keepdims=True)
        ok = jnp.logical_and(mine, jnp.broadcast_to(chosen, (heads, 128)) > 0)
        bias[b] = jnp.where(ok, 0.0, NEGATIVE)

    reps = CHUNK // 128
    col = lax.broadcasted_iota(jnp.int32, (1, CHUNK), 1) // kv_heads
    dims = (((1,), (1,)), ((), ()))
    top = jnp.full((heads, 128), 3 * NEGATIVE, jnp.float32)
    for b in range(blocks_here):
        k_copies[b].wait()
        start = (me * blocks_here + b) * BLOCK
        for j in range(span // CHUNK):
            lo = b * span + j * CHUNK
            s = lax.dot_general(q, kbuf[lo : lo + CHUNK, :], dims, preferred_element_type=jnp.float32)
            end = jnp.where(col + (start + j * (CHUNK // kv_heads)) < length, 0.0, NEGATIVE)
            for r in range(reps):
                part = s[:, r * 128 : (r + 1) * 128] + (bias[b] + end[:, r * 128 : (r + 1) * 128])
                top = jnp.maximum(top, part)
                sbuf[:, lo + r * 128 : lo + (r + 1) * 128] = part
    high = jnp.max(top, axis=1, keepdims=True)
    high_wide = jnp.broadcast_to(high, (heads, 128))

    total = jnp.zeros((heads, 128), jnp.float32)
    acc = jnp.zeros((heads, hd), jnp.float32)
    for b in range(blocks_here):
        v_copies[b].wait()
        for j in range(span // CHUNK):
            lo = b * span + j * CHUNK
            pieces = []
            for r in range(reps):
                w = jnp.exp2((sbuf[:, lo + r * 128 : lo + (r + 1) * 128] - high_wide) * factor)
                total = total + w
                pieces.append(w.astype(jnp.bfloat16))
            acc = acc + jnp.dot(
                jnp.concatenate(pieces, axis=1), vbuf[lo : lo + CHUNK, :], preferred_element_type=jnp.float32
            )
    total_wide = jnp.broadcast_to(jnp.sum(total, axis=1, keepdims=True), (heads, 128))
    half = lax.broadcasted_iota(jnp.int32, (heads, 128), 1) < 64
    stats = jnp.where(half, high_wide, total_wide)
    for p in range(n):
        msg[p, 0] = acc[p * hl : (p + 1) * hl, :]
        msg[p, 1] = stats[p * hl : (p + 1) * hl, :]
    backs = []
    for d in range(1, n):
        peer = lax.rem(me + d, n)
        c = pltpu.make_async_remote_copy(
            src_ref=msg.at[peer],
            dst_ref=came.at[me],
            send_sem=m_send.at[d],
            recv_sem=m_recv.at[d],
            device_id={"seq": peer},
            device_id_type=pl.DeviceIdType.MESH,
        )
        c.start()
        backs.append(c)
    came[me] = msg[me]
    for c in sends:
        c.wait_send()
    for c in backs:
        c.wait_recv()
    best = came[0, 1]
    for p in range(1, n):
        best = jnp.maximum(best, came[p, 1])
    best = jnp.broadcast_to(best[:, 0:1], (hl, 128))
    sum_out = jnp.zeros((hl, hd), jnp.float32)
    sum_total = jnp.zeros((hl, 128), jnp.float32)
    for p in range(n):
        st = came[p, 1]
        scale = jnp.exp2((jnp.broadcast_to(st[:, 0:1], (hl, 128)) - best) * factor)
        sum_out = sum_out + came[p, 0] * scale
        sum_total = sum_total + jnp.broadcast_to(st[:, 64:65], (hl, 128)) * scale
    out_ref[0] = (sum_out / sum_total).astype(out_ref.dtype)
    for c in backs:
        c.wait_send()


def shards(n, queries, keys, values, picks, lengths):
    _, hl, hd = queries.shape
    _, local_len, kv_heads, _ = keys.shape
    heads = n * hl
    cols = local_len * kv_heads
    blocks_here = local_len // BLOCK
    k2 = keys.reshape(cols, hd)
    v2 = values.reshape(cols, hd)
    any_space = pl.BlockSpec(memory_space=pl.ANY)
    sems = [pltpu.SemaphoreType.DMA((n,)) for _ in range(6)]
    return pl.pallas_call(
        functools.partial(kernel, n, kv_heads),
        out_shape=pltpu.VMEM((1, hl, hd), jnp.bfloat16),
        in_specs=[pl.BlockSpec(memory_space=pltpu.HBM)] + [any_space] * 4,
        out_specs=pl.BlockSpec(memory_space=pltpu.VMEM),
        scratch_shapes=[
            pltpu.VMEM((cols, hd), jnp.bfloat16),
            pltpu.VMEM((cols, hd), jnp.bfloat16),
            pltpu.VMEM((n, hl, hd), jnp.bfloat16),
            pltpu.VMEM((n, picks.shape[2], 1, hl), jnp.int32),
            pltpu.VMEM((heads, hd), jnp.float32),
            pltpu.VMEM((8, 128), jnp.int32),
            pltpu.SMEM((1,), jnp.int32),
            pltpu.VMEM((blocks_here, heads, 128), jnp.float32),
            pltpu.VMEM((heads, cols), jnp.float32),
            pltpu.VMEM((n, 2, hl, 128), jnp.float32),
            pltpu.VMEM((n, 2, hl, 128), jnp.float32),
            pltpu.SemaphoreType.DMA((blocks_here,)),
            pltpu.SemaphoreType.DMA((blocks_here,)),
            pltpu.SemaphoreType.DMA((3,)),
        ]
        + sems,
        compiler_params=pltpu.CompilerParams(collective_id=0, has_side_effects=True),
        name="block_attention",
    )(lengths, queries, jnp.transpose(picks, (2, 0, 1)), k2, v2)


def solution(mesh):
    return jax.shard_map(
        functools.partial(shards, mesh.shape["seq"]),
        mesh=mesh,
        in_specs=(
            P(("grp", "kv"), "seq", None),
            P(("grp", "kv"), "seq", None, None),
            P(("grp", "kv"), "seq", None, None),
            P(("grp", "kv"), "seq", None),
            P(("grp", "kv")),
        ),
        out_specs=P(("grp", "kv"), "seq", None),
        check_vma=False,
    )
```

```python
import functools
import math

import jax
import jax.numpy as jnp
from jax import lax
from jax.experimental import pallas as pl
from jax.experimental.pallas import tpu as pltpu
from jax.sharding import PartitionSpec as P

BLOCK = 512
MIX = 256
NEGATIVE = -1e30


def kernel(
    n,
    kv_heads,
    lengths_ref,
    q_ref,
    picks_ref,
    k_hbm,
    v_hbm,
    out_ref,
    kbuf,
    vbuf,
    qbuf,
    pbuf,
    qall,
    pall,
    lbuf,
    khead,
    vhead,
    msg,
    came,
    k_sem,
    v_sem,
    own_sem,
    q_send,
    q_recv,
    p_send,
    p_recv,
    m_send,
    m_recv,
):
    me = lax.axis_index("seq")
    hl, hd = q_ref.shape[1], q_ref.shape[2]
    heads = n * hl
    group = heads // kv_heads
    span = BLOCK * kv_heads
    blocks_here = k_hbm.shape[0] // span
    factor = math.log2(math.e) / math.sqrt(hd)

    barrier = pltpu.get_barrier_semaphore()
    for d in range(1, n):
        pl.semaphore_signal(
            barrier, inc=1, device_id={"seq": lax.rem(me + d, n)}, device_id_type=pl.DeviceIdType.MESH
        )
    k_copies, v_copies = [], []
    for b in range(blocks_here):
        rows = pl.ds(b * span, span)
        k_copies.append(pltpu.make_async_copy(k_hbm.at[rows], kbuf.at[rows], k_sem.at[b]))
        v_copies.append(pltpu.make_async_copy(v_hbm.at[rows], vbuf.at[rows], v_sem.at[b]))
    for c in k_copies:
        c.start()
    own_q = pltpu.make_async_copy(q_ref.at[0], qbuf.at[me], own_sem.at[0])
    own_p = pltpu.make_async_copy(picks_ref, pbuf.at[me], own_sem.at[1])
    own_l = pltpu.make_async_copy(lengths_ref, lbuf, own_sem.at[2])
    own_q.start()
    own_p.start()
    own_l.start()
    for c in v_copies:
        c.start()
    pall[...] = jnp.full(pall.shape, -1, jnp.int32)
    own_q.wait()
    own_p.wait()
    own_l.wait()
    pl.semaphore_wait(barrier, n - 1)

    sends = {}
    for d in reversed(range(1, n)):
        peer = {"seq": lax.rem(me + d, n)}
        for name, buf, s_sem, r_sem in (("q", qbuf, q_send, q_recv), ("p", pbuf, p_send, p_recv)):
            c = pltpu.make_async_remote_copy(
                src_ref=buf.at[me],
                dst_ref=buf.at[me],
                send_sem=s_sem.at[d],
                recv_sem=r_sem.at[me],
                device_id=peer,
                device_id_type=pl.DeviceIdType.MESH,
            )
            c.start()
            sends[name, d] = c

    row = lax.broadcasted_iota(jnp.int32, (MIX, MIX), 0)
    lane = lax.broadcasted_iota(jnp.int32, (MIX, MIX), 1)
    tall = MIX // kv_heads
    perm = jnp.where(lane == (row % tall) * kv_heads + row // tall, 1.0, 0.0).astype(jnp.bfloat16)

    def regroup(src, dst, b):
        def step(i, carry):
            lo = pl.multiple_of(b * span + i * 2 * MIX, 2 * MIX)
            t0 = pl.multiple_of(b * BLOCK + i * 2 * tall, 2 * tall)
            x = jnp.concatenate([src[pl.ds(lo, MIX), :], src[pl.ds(lo + MIX, MIX), :]], axis=1)
            y = jnp.dot(perm, x, preferred_element_type=jnp.float32).astype(jnp.bfloat16)
            hd = src.shape[1]
            for k in range(kv_heads):
                dst[k, pl.ds(t0, tall), :] = y[k * tall : (k + 1) * tall, :hd]
                dst[k, pl.ds(t0 + tall, tall), :] = y[k * tall : (k + 1) * tall, hd:]
            return carry

        lax.fori_loop(0, span // (2 * MIX), step, 0, unroll=8)

    for b in range(blocks_here):
        k_copies[b].wait()
        regroup(kbuf, khead, b)
    for b in range(blocks_here):
        v_copies[b].wait()
        regroup(vbuf, vhead, b)

    length = lbuf[0]
    owners = group // hl
    local_len = blocks_here * BLOCK
    dims = (((1,), (1,)), ((), ()))
    wide = lax.broadcasted_iota(jnp.int32, (group, BLOCK), 1)
    half = lax.broadcasted_iota(jnp.int32, (group, 128), 1) < 64
    for k in range(kv_heads):
        for i in range(owners):
            p = k * owners + i

            @pl.when(p != me)
            def _():
                for buf, s_sem, r_sem in ((qbuf, q_send, q_recv), (pbuf, p_send, p_recv)):
                    pltpu.make_async_remote_copy(
                        src_ref=buf.at[p],
                        dst_ref=buf.at[p],
                        send_sem=s_sem.at[0],
                        recv_sem=r_sem.at[p],
                        device_id={"seq": lax.rem(me + 1, n)},
                        device_id_type=pl.DeviceIdType.MESH,
                    ).wait_recv()

            qall[k, i * hl : (i + 1) * hl, :] = qbuf[p].astype(jnp.float32)
            pall[k, 0 : pbuf.shape[1], i * hl : (i + 1) * hl] = pbuf[p, :, 0, :]
        q = qall[k].astype(jnp.bfloat16)
        picks = jnp.transpose(pall[k])[0:group, :]
        s = lax.dot_general(q, khead[k], dims, preferred_element_type=jnp.float32)
        parts = []
        high = jnp.full((group, 1), NEGATIVE, jnp.float32)
        for b in range(blocks_here):
            block_id = me * blocks_here + b
            chosen = jnp.max((picks == block_id).astype(jnp.int32), axis=1, keepdims=True)
            limit = jnp.where(chosen > 0, length - block_id * BLOCK, 0)
            part = jnp.where(wide < limit, s[:, b * BLOCK : (b + 1) * BLOCK], NEGATIVE)
            high = jnp.maximum(high, jnp.max(part, axis=1, keepdims=True))
            parts.append(part)
        w = jnp.exp2((jnp.concatenate(parts, axis=1) - high) * factor)
        total = jnp.sum(w, axis=1, keepdims=True)
        acc = jnp.dot(w.astype(jnp.bfloat16), vhead[k], preferred_element_type=jnp.float32)
        stats = jnp.where(half, jnp.broadcast_to(high, (group, 128)), jnp.broadcast_to(total, (group, 128)))
        for i in range(owners):
            p = k * owners + i
            msg[p, 0] = acc[i * hl : (i + 1) * hl, :]
            msg[p, 1] = stats[i * hl : (i + 1) * hl, :]

            @pl.when(p != me)
            def _():
                pltpu.make_async_remote_copy(
                    src_ref=msg.at[p],
                    dst_ref=came.at[me],
                    send_sem=m_send.at[p],
                    recv_sem=m_recv.at[me],
                    device_id={"seq": p},
                    device_id_type=pl.DeviceIdType.MESH,
                ).start()

    def back(d):
        p = lax.rem(me + d, n)
        return pltpu.make_async_remote_copy(
            src_ref=msg.at[p],
            dst_ref=came.at[p],
            send_sem=m_send.at[p],
            recv_sem=m_recv.at[p],
            device_id={"seq": p},
            device_id_type=pl.DeviceIdType.MESH,
        )

    backs = [back(d) for d in range(1, n)]
    came[me] = msg[me]
    for c in sends.values():
        c.wait_send()
    for c in backs:
        c.wait_recv()
    best = came[0, 1]
    for p in range(1, n):
        best = jnp.maximum(best, came[p, 1])
    best = jnp.broadcast_to(best[:, 0:1], (hl, 128))
    sum_out = jnp.zeros((hl, hd), jnp.float32)
    sum_total = jnp.zeros((hl, 128), jnp.float32)
    for p in range(n):
        st = came[p, 1]
        scale = jnp.exp2((jnp.broadcast_to(st[:, 0:1], (hl, 128)) - best) * factor)
        sum_out = sum_out + came[p, 0] * scale
        sum_total = sum_total + jnp.broadcast_to(st[:, 64:65], (hl, 128)) * scale
    out_ref[0] = (sum_out / sum_total).astype(out_ref.dtype)
    for c in backs:
        c.wait_send()


def shards(n, queries, keys, values, picks, lengths):
    _, hl, hd = queries.shape
    _, local_len, kv_heads, _ = keys.shape
    heads = n * hl
    cols = local_len * kv_heads
    blocks_here = local_len // BLOCK
    k2 = keys.reshape(cols, hd)
    v2 = values.reshape(cols, hd)
    any_space = pl.BlockSpec(memory_space=pl.ANY)
    sems = [pltpu.SemaphoreType.DMA((n,)) for _ in range(6)]
    return pl.pallas_call(
        functools.partial(kernel, n, kv_heads),
        out_shape=pltpu.VMEM((1, hl, hd), jnp.bfloat16),
        in_specs=[pl.BlockSpec(memory_space=pltpu.HBM)] + [any_space] * 4,
        out_specs=pl.BlockSpec(memory_space=pltpu.VMEM),
        scratch_shapes=[
            pltpu.VMEM((cols, hd), jnp.bfloat16),
            pltpu.VMEM((cols, hd), jnp.bfloat16),
            pltpu.VMEM((n, hl, hd), jnp.bfloat16),
            pltpu.VMEM((n, picks.shape[2], 1, hl), jnp.int32),
            pltpu.VMEM((kv_heads, heads // kv_heads, hd), jnp.float32),
            pltpu.VMEM((kv_heads, 8, 128), jnp.int32),
            pltpu.SMEM((1,), jnp.int32),
            pltpu.VMEM((kv_heads, local_len, hd), jnp.bfloat16),
            pltpu.VMEM((kv_heads, local_len, hd), jnp.bfloat16),
            pltpu.VMEM((n, 2, hl, 128), jnp.float32),
            pltpu.VMEM((n, 2, hl, 128), jnp.float32),
            pltpu.SemaphoreType.DMA((blocks_here,)),
            pltpu.SemaphoreType.DMA((blocks_here,)),
            pltpu.SemaphoreType.DMA((3,)),
        ]
        + sems,
        compiler_params=pltpu.CompilerParams(collective_id=0, has_side_effects=True),
        name="block_attention",
    )(lengths, queries, jnp.transpose(picks, (2, 0, 1)), k2, v2)


def solution(mesh):
    return jax.shard_map(
        functools.partial(shards, mesh.shape["seq"]),
        mesh=mesh,
        in_specs=(
            P(("grp", "kv"), "seq", None),
            P(("grp", "kv"), "seq", None, None),
            P(("grp", "kv"), "seq", None, None),
            P(("grp", "kv"), "seq", None),
            P(("grp", "kv")),
        ),
        out_specs=P(("grp", "kv"), "seq", None),
        check_vma=False,
    )
```
